32 devices in a mesh: seq: 8 (over z, y), batch: 4 (over x, core).
Axes of the slice: x: 2, y: 2, z: 4, core: 2. Of those that a mesh axis runs over, the one named last changes fastest.
Arguments:
- queries: bfloat16 [4, 1024, 4096], P('batch', 'seq'), may hold values from -130 to 130
- keys: bfloat16 [4, 1024, 1024], P('batch', 'seq'), may hold values from -4 to 4
- values: bfloat16 [4, 1024, 1024], P('batch', 'seq'), may hold values from -4 to 4
- lengths: int32 [4], P('batch'), may hold values from 512 to 1024
- block_pos: int32 [4, 8], P('batch'), may hold values from 0 to 7, each once within a row
- w_in: bfloat16 [6144, 1024], replicated, may hold values from -0.078125 to 0.078125
- b_in: float32 [1024], replicated, may hold values from -3 to 3
- output_weight: bfloat16 [1024, 8], replicated, may hold values from -0.1875 to 0.1875
- output_bias: float32 [8], replicated, may hold values from 1 to 2
Outputs:
- grad_w_in: float32 [6144, 1024], P(('seq', 'batch'))
- grad_b_in: float32 [1024], replicated
- output_weight_gradient: float32 [1024, 8], replicated
- output_bias_gradient: float32 [8], replicated
The draws below stay inside these ranges and needn't reach their ends.
Inputs may be any that keep to these rules, and one draw needn't show every extreme that they name: Each row of block_pos names every block 0 to 7 once.
All inputs are finite; a program needn't handle non-finite values.
Results may differ from the reference program's by a relative error of at most 0.0017.
The reference program's roundings to bfloat16 on the way (of `features`, `act`, `resid` and `delta`) count: a program that leaves them out, or rounds other values in their place, can miss the bound.
Values may be sent and summed in bfloat16 or wider, within the bound.
A program may use at most 128 MiB of HBM per device.

```python
import math
import jax
import jax.numpy as jnp
from jax import lax

QUERY_HEADS = 32
KEY_VALUE_HEADS = 8
HEAD_DIMENSION = 128
HIDDEN_UNITS = 1024
SEQ_DEV = 128
KD = 1024
FEAT = 6144
TOKEN_COUNT = 1024
SEQUENCE_COUNT = 4
N_SEQ = 8


def group_keys(key):
    base_offset = jax.random.fold_in(key, 7301)
    return jnp.clip(jax.random.normal(base_offset, (SEQUENCE_COUNT, TOKEN_COUNT, KEY_VALUE_HEADS * HEAD_DIMENSION), jnp.float32), -4.0, 4.0)


def draw_keys(key, part):
    base_offset = group_keys(key)
    return base_offset.astype(jnp.bfloat16)


def draw_queries(key, part):
    fresh = jax.random.fold_in(key, 1709)
    base_offset = jnp.clip(jax.random.normal(fresh, (SEQUENCE_COUNT, TOKEN_COUNT, QUERY_HEADS * HEAD_DIMENSION), jnp.float32), -4.0, 4.0)
    return base_offset.astype(jnp.bfloat16)


def place_ends(entries, stream_key, least, largest):
    index_at = [jax.random.randint(jax.random.fold_in(stream_key, axis), (), 0, length) for axis, length in enumerate(entries.shape)]
    widest = entries.shape.index(max(entries.shape))
    next_to = index_at[:widest] + [(index_at[widest] + 1) % entries.shape[widest]] + index_at[widest + 1:]
    return entries.at[tuple(index_at)].set(least).at[tuple(next_to)].set(largest)


def shard_levels(stream_key, shape, pieces, least, high):
    gain = 1.0
    for dim, blocks in pieces:
        steps = jax.random.uniform(jax.random.fold_in(jax.random.fold_in(stream_key, 6), dim), (blocks,), jnp.float32, least / len(pieces), high / len(pieces))
        gain = gain * jnp.repeat(jnp.exp(steps), shape[dim] // blocks).reshape((-1,) + (1,) * (len(shape) - 1 - dim))
    return gain


def bell_draw(stream_key, dims, scale, most, split=(), kind=jnp.bfloat16):
    array = jax.random.normal(stream_key, dims, jnp.float32) * scale
    if len(split) > 0:
        array = shard_levels(stream_key, dims, split, -0.22, 0.18) * array
    return jnp.clip(array, min=-most, max=most).astype(kind)


def setup_inputs(seed: int = 0) -> dict:
    seeds = jax.random.split(jax.random.key(seed), 10)
    queries = draw_queries(jax.random.fold_in(seeds[9], 71), 0)
    keys = draw_keys(jax.random.fold_in(seeds[9], 71), 0)
    values = bell_draw(seeds[2], (SEQUENCE_COUNT, TOKEN_COUNT, KD), 1.0, 4.0, ((0, 4), (1, 8)))
    lengths = place_ends(jax.random.randint(seeds[3], (SEQUENCE_COUNT,), TOKEN_COUNT // 2, TOKEN_COUNT + 1), jax.random.fold_in(seeds[3], 1), TOKEN_COUNT // 2, TOKEN_COUNT).astype(jnp.int32)
    block_pos = jax.vmap(lambda own: jax.random.permutation(own, N_SEQ))(jax.random.split(seeds[4], SEQUENCE_COUNT)).reshape((SEQUENCE_COUNT, N_SEQ)).astype(jnp.int32)
    w_in = bell_draw(seeds[5], (FEAT, HIDDEN_UNITS), FEAT ** -0.5, 0.078125)
    b_in = bell_draw(seeds[6], (HIDDEN_UNITS,), 0.5, 3.0, (), jnp.float32)
    output_weight = bell_draw(seeds[7], (HIDDEN_UNITS, KEY_VALUE_HEADS), HIDDEN_UNITS ** -0.5, 0.1875)
    output_bias = jnp.clip(jax.random.uniform(seeds[8], (KEY_VALUE_HEADS,), jnp.float32, 1.0, 2.0), 1.0, 2.0)
    return {"queries": queries, "keys": keys, "values": values, "lengths": lengths, "block_pos": block_pos, "w_in": w_in, "b_in": b_in, "output_weight": output_weight, "output_bias": output_bias}


def column_mass(q_rows, k_rows, positions, limit):
    group_index = QUERY_HEADS // KEY_VALUE_HEADS
    scale = 1.0 / math.sqrt(HEAD_DIMENSION)

    def queries_per_group(g, sums):
        g32 = jnp.asarray(g).astype(jnp.int32)
        k_part = lax.dynamic_slice_in_dim(k_rows, g32 * HEAD_DIMENSION, HEAD_DIMENSION, 1).astype(jnp.float32)
        key_live = positions < limit

        def per_block(i, column):
            i32 = jnp.asarray(i).astype(jnp.int32)
            start = i32 * SEQ_DEV
            q_part = lax.dynamic_slice(q_rows, (start, g32 * group_index * HEAD_DIMENSION), (SEQ_DEV, group_index * HEAD_DIMENSION))
            q_part = q_part.astype(jnp.float32).reshape(SEQ_DEV, group_index, HEAD_DIMENSION)
            q_pos = lax.dynamic_slice_in_dim(positions, start, SEQ_DEV)
            allowed = (positions[None, :] <= q_pos[:, None]) & key_live[None, :]
            scores = jnp.einsum('qhd,kd->hqk', q_part, k_part) * scale
            masked = jnp.where(allowed[None], scores, -1e+30)
            top = lax.optimization_barrier(jnp.max(masked, axis=2, keepdims=True))
            weights = jnp.where(allowed[None], jnp.exp(masked - top), 0.0)
            total = lax.optimization_barrier(jnp.sum(weights, axis=2, keepdims=True))
            q_live = (q_pos < limit).astype(jnp.float32)
            share = weights / total * q_live[None, :, None]
            return column + lax.optimization_barrier(jnp.sum(share, axis=(0, 1)))
        column = lax.fori_loop(0, N_SEQ, per_block, jnp.zeros((TOKEN_COUNT,), jnp.float32))
        return lax.dynamic_update_index_in_dim(sums, column, g32, 0)
    return lax.fori_loop(0, KEY_VALUE_HEADS, queries_per_group, jnp.zeros((KEY_VALUE_HEADS, TOKEN_COUNT), jnp.float32))

def reference(queries, keys, values, lengths, block_pos, w_in, b_in, output_weight, output_bias):
    norm = 1.0 / math.sqrt(SEQUENCE_COUNT * TOKEN_COUNT)
    offsets = jnp.arange(SEQ_DEV, dtype=jnp.int32)
    grad_w_in = jnp.zeros((FEAT, HIDDEN_UNITS), jnp.float32)
    grad_b_in = jnp.zeros((HIDDEN_UNITS,), jnp.float32)
    output_weight_gradient = jnp.zeros((HIDDEN_UNITS, KEY_VALUE_HEADS), jnp.float32)
    output_bias_gradient = jnp.zeros((KEY_VALUE_HEADS,), jnp.float32)
    for index in range(SEQUENCE_COUNT):
        q_rows = queries[index]
        k_rows = keys[index]
        v_rows = values[index]
        positions = (block_pos[index][:, None] * SEQ_DEV + offsets[None, :]).reshape(-1).astype(jnp.int32)
        limit = lengths[index]
        live = (positions < limit).astype(jnp.float32)
        mass = column_mass(q_rows, k_rows, positions, limit)
        labels = jnp.log1p(mass).T
        features = jnp.concatenate([q_rows, k_rows, v_rows], axis=1)
        pre = jnp.dot(features, w_in, preferred_element_type=jnp.float32) + b_in
        act = jax.nn.silu(pre).astype(jnp.bfloat16)
        pred = jnp.dot(act, output_weight, preferred_element_type=jnp.float32) + output_bias
        resid = ((pred - labels) * live[:, None] * norm).astype(jnp.bfloat16)
        back = jnp.dot(resid, output_weight.T, preferred_element_type=jnp.float32)
        sig = jax.nn.sigmoid(pre)
        delta = (back * sig * (1.0 + pre * (1.0 - sig))).astype(jnp.bfloat16)
        grad_w_in = grad_w_in + jnp.dot(features.T, delta, preferred_element_type=jnp.float32)
        grad_b_in = grad_b_in + lax.optimization_barrier(jnp.sum(delta.astype(jnp.float32), axis=0))
        output_weight_gradient = output_weight_gradient + jnp.dot(act.T, resid, preferred_element_type=jnp.float32)
        output_bias_gradient = output_bias_gradient + lax.optimization_barrier(jnp.sum(resid.astype(jnp.float32), axis=0))
    return (grad_w_in, grad_b_in, output_weight_gradient, output_bias_gradient)
```

```python
import functools
import math

import jax
import jax.numpy as jnp
from jax import lax
from jax.experimental import pallas as pl
from jax.experimental.pallas import tpu as pltpu
from jax.sharding import PartitionSpec as P

F32 = jnp.float32
BF16 = jnp.bfloat16
MESH = pl.DeviceIdType.MESH


def copy_to(src, dst, send, recv, target):
    return pltpu.make_async_remote_copy(
        src_ref=src,
        dst_ref=dst,
        send_sem=send,
        recv_sem=recv,
        device_id=target,
        device_id_type=MESH,
    )


def kernel(
    n,
    nb,
    norm,
    scale,
    q_ref,
    k_ref,
    feat_ref,
    pre_ref,
    wt_ref,
    bias_ref,
    kpos_ref,
    qpos_ref,
    live_col_ref,
    live_row_ref,
    limit_ref,
    grad_ref,
    gb_ref,
    gw_ref,
    kg,
    ft,
    act,
    msum,
    mp,
    mr,
    delta,
    dg,
    otc,
    otr,
    obs,
    obr,
    ofin,
    dbs,
    dbr,
    cs,
    cr,
    ksem,
    fsem,
    msem,
    dsem,
    osem,
    bsem,
    gsem,
    hsem,
    csem,
):
    me = lax.axis_index("seq")
    mb = lax.axis_index("batch")
    rows, kd = k_ref.shape
    heads = msum.shape[0]
    head = kd // heads
    per_group = q_ref.shape[1] // kd
    hidden = pre_ref.shape[1]
    inner = 2
    outer = n // inner
    mo = me // inner
    mi = me % inner
    pair = mo * inner + (inner - 1 - mi)

    def seq_peer(d):
        return lax.rem(me + d, n)

    def batch_peer(d):
        return lax.rem(mb + d, nb)

    def outer_peer(d):
        return lax.rem(mo + d, outer) * inner + mi

    def outer_source(d):
        return lax.rem(mo - d + outer, outer) * inner + mi

    barrier = pltpu.get_barrier_semaphore()
    for d in range(1, n):
        pl.semaphore_signal(barrier, inc=1, device_id={"seq": seq_peer(d)}, device_id_type=MESH)
    for d in range(1, nb):
        pl.semaphore_signal(
            barrier, inc=1, device_id={"batch": batch_peer(d)}, device_id_type=MESH
        )
    pl.semaphore_wait(barrier, n + nb - 2)

    def block(ref, owner):
        return ref.at[pl.ds(pl.multiple_of(owner * rows, rows), rows)]

    def gather_start(src, dst, sem):
        copies = []
        for d in range(1, outer):
            copy = copy_to(
                src, block(dst, me), sem.at[0, d], sem.at[1, d], {"seq": outer_peer(d)}
            )
            copy.start()
            copies.append(copy)
        copy = copy_to(src, block(dst, me), sem.at[2, 0], sem.at[3, 0], {"seq": pair})
        copy.start()
        return copies, [copy]

    def gather_finish(dst, sem, started):
        direct, passed = started
        for d in range(1, outer):
            direct[d - 1].wait_recv()
            held = block(dst, outer_source(d))
            copy = copy_to(held, held, sem.at[2, d], sem.at[3, d], {"seq": pair})
            copy.start()
            passed.append(copy)
        for copy in passed:
            copy.wait_recv()
        return direct + passed

    key_copies = gather_start(k_ref, kg, ksem)
    feat_copies = []
    for d in range(1, n):
        copy = copy_to(
            feat_ref.at[seq_peer(d)],
            ft.at[:, pl.ds(pl.multiple_of(me * rows, rows), rows)],
            fsem.at[0, d],
            fsem.at[1, d],
            {"seq": seq_peer(d)},
        )
        copy.start()
        feat_copies.append(copy)
    kg[pl.ds(pl.multiple_of(me * rows, rows), rows), :] = k_ref[...]
    ft[:, pl.ds(pl.multiple_of(me * rows, rows), rows)] = feat_ref[me]
    pre = pre_ref[...]
    act[...] = (pre * jax.nn.sigmoid(pre)).astype(BF16)
    sent = gather_finish(kg, ksem, key_copies)

    limit = limit_ref[0]

    def group(g, carry):
        keys = kg[:, pl.ds(pl.multiple_of(g * head, head), head)]
        kpos = kpos_ref[...]
        allowed = (kpos <= qpos_ref[...]) & (kpos < limit)
        column = jnp.zeros((1, n * rows), F32)
        for j in range(per_group):
            start = pl.multiple_of((g * per_group + j) * head, head)
            score = lax.dot_general(
                q_ref[:, pl.ds(start, head)],
                keys,
                (((1,), (1,)), ((), ())),
                preferred_element_type=F32,
            )
            masked = jnp.where(allowed, score * scale, -1e30)
            top = jnp.max(masked, axis=1, keepdims=True)
            weights = jnp.exp(masked - top)
            denom = jnp.sum(weights, axis=1, keepdims=True)
            column += jnp.sum(weights * (live_col_ref[...] / denom), axis=0, keepdims=True)
        msum[g] = column
        return carry

    lax.fori_loop(0, heads, group, 0)
    for p in range(n):
        mp[p] = msum[:, 0, p * rows : (p + 1) * rows]
    mass_copies = []
    for d in range(1, n):
        copy = copy_to(
            mp.at[seq_peer(d)], mr.at[d], msem.at[0, d], msem.at[1, d], {"seq": seq_peer(d)}
        )
        copy.start()
        mass_copies.append(copy)
    wt = wt_ref[...]
    pred = (
        lax.dot_general(wt, act[...], (((1,), (1,)), ((), ())), preferred_element_type=F32)[:heads]
        + bias_ref[...]
    )
    mass = mp[me]
    for d in range(1, n):
        mass_copies[d - 1].wait_recv()
        mass = mass + mr[d]
    sent += mass_copies
    resid = ((pred - jnp.log1p(mass)) * live_row_ref[...] * norm).astype(BF16)
    resid32 = resid.astype(F32)
    resid_all = jnp.concatenate([resid32, jnp.zeros_like(resid32)], axis=0)
    resid_t = resid_all.T.astype(BF16)
    back = jnp.dot(resid_t, wt, preferred_element_type=F32)
    pre = pre_ref[...]
    sig = jax.nn.sigmoid(pre)
    delta[...] = (back * sig * (1.0 + pre * (1.0 - sig))).astype(BF16)
    delta_copies = gather_start(delta, dg, dsem)
    dg[pl.ds(pl.multiple_of(me * rows, rows), rows), :] = delta[...]

    out_term = jnp.dot(resid_all.astype(BF16), act[...], preferred_element_type=F32)
    width = hidden // n
    bias_sum = jnp.broadcast_to(jnp.sum(resid32, axis=1, keepdims=True), (heads, width))
    for p in range(n):
        otc[p, :heads] = out_term[:heads, p * width : (p + 1) * width]
        otc[p, heads:] = bias_sum
    first = []
    for d in range(1, n):
        copy = copy_to(
            otc.at[seq_peer(d)], otr.at[d], osem.at[0, d], osem.at[1, d], {"seq": seq_peer(d)}
        )
        copy.start()
        first.append(copy)
    small = otc[me]
    for d in range(1, n):
        first[d - 1].wait_recv()
        small = small + otr[d]
    obs[...] = small
    second = []
    for d in range(1, nb):
        copy = copy_to(
            obs, obr.at[d], bsem.at[0, d], bsem.at[1, d], {"batch": batch_peer(d)}
        )
        copy.start()
        second.append(copy)

    sent += gather_finish(dg, dsem, delta_copies)
    for copy in feat_copies:
        copy.wait_recv()
    part = cs.shape[1]
    chunks = []
    for d in range(1, nb):
        start = pl.multiple_of(batch_peer(d) * part, 16)
        cs[d] = jnp.dot(ft[pl.ds(start, part), :], dg[...], preferred_element_type=F32)
        copy = copy_to(
            cs.at[d], cr.at[d], csem.at[0, d], csem.at[1, d], {"batch": batch_peer(d)}
        )
        copy.start()
        chunks.append(copy)
    dbs[...] = jnp.dot(jnp.ones((8, n * rows), BF16), dg[...], preferred_element_type=F32)
    sums = []
    for d in range(1, nb):
        copy = copy_to(
            dbs, dbr.at[d], gsem.at[0, d], gsem.at[1, d], {"batch": batch_peer(d)}
        )
        copy.start()
        sums.append(copy)

    small = obs[...]
    for d in range(1, nb):
        second[d - 1].wait_recv()
        small = small + obr[d]
    ofin[me] = small
    third = []
    for d in range(1, n):
        copy = copy_to(
            ofin.at[me], ofin.at[me], hsem.at[0, d], hsem.at[1, d], {"seq": seq_peer(d)}
        )
        copy.start()
        third.append(copy)
    start = pl.multiple_of(mb * part, 16)
    total = jnp.dot(ft[pl.ds(start, part), :], dg[...], preferred_element_type=F32)
    for d in range(1, nb):
        chunks[d - 1].wait_recv()
        total = total + cr[d]
    grad_ref[...] = total
    grad_b = dbs[...]
    for d in range(1, nb):
        sums[d - 1].wait_recv()
        grad_b = grad_b + dbr[d]
    gb_ref[...] = grad_b
    for copy in third:
        copy.wait_recv()
    gw_ref[...] = ofin[...]
    for copy in sent + feat_copies + first + second + chunks + sums + third:
        copy.wait_send()


def on_device(queries, keys, values, lengths, block_pos, w_in, b_in, output_weight, output_bias):
    n = lax.axis_size("seq")
    nb = lax.axis_size("batch")
    q_rows = queries[0]
    k_rows = keys[0]
    v_rows = values[0]
    rows, kd = k_rows.shape
    heads = output_weight.shape[1]
    hidden = w_in.shape[1]
    feat = w_in.shape[0]
    cols = feat // n
    part = cols // nb
    scale = 1.0 / math.sqrt(kd // heads)
    norm = 1.0 / math.sqrt(nb * n * rows)
    order = block_pos[0]
    offsets = jnp.arange(rows, dtype=jnp.int32)
    key_pos = (order[:, None] * rows + offsets[None, :]).reshape(1, -1)
    mine = lax.axis_index("seq")
    query_pos = lax.dynamic_index_in_dim(order, mine, 0, keepdims=False) * rows + offsets
    live = (query_pos < lengths[0]).astype(F32)
    features = jnp.concatenate([q_rows, k_rows, v_rows], axis=1)
    pre = jnp.dot(features, w_in, preferred_element_type=F32) + b_in
    turned = features.T.reshape(n, cols, rows)
    wt = jnp.pad(output_weight.T, ((0, heads), (0, 0)))
    vmem = pl.BlockSpec(memory_space=pltpu.VMEM)
    total = n * rows
    width = hidden // n
    grad, gb, gw = pl.pallas_call(
        functools.partial(kernel, n, nb, norm, scale),
        out_shape=(
            jax.ShapeDtypeStruct((part, hidden), F32),
            jax.ShapeDtypeStruct((8, hidden), F32),
            jax.ShapeDtypeStruct((n, 2 * heads, width), F32),
        ),
        in_specs=[vmem] * 10 + [pl.BlockSpec(memory_space=pltpu.SMEM)],
        out_specs=(vmem, vmem, vmem),
        scratch_shapes=[
            pltpu.VMEM((total, kd), BF16),
            pltpu.VMEM((cols, total), BF16),
            pltpu.VMEM((rows, hidden), BF16),
            pltpu.VMEM((heads, 1, total), F32),
            pltpu.VMEM((n, heads, rows), F32),
            pltpu.VMEM((n, heads, rows), F32),
            pltpu.VMEM((rows, hidden), BF16),
            pltpu.VMEM((total, hidden), BF16),
            pltpu.VMEM((n, 2 * heads, width), F32),
            pltpu.VMEM((n, 2 * heads, width), F32),
            pltpu.VMEM((2 * heads, width), F32),
            pltpu.VMEM((nb, 2 * heads, width), F32),
            pltpu.VMEM((n, 2 * heads, width), F32),
            pltpu.VMEM((8, hidden), F32),
            pltpu.VMEM((nb, 8, hidden), F32),
            pltpu.VMEM((nb, part, hidden), F32),
            pltpu.VMEM((nb, part, hidden), F32),
            pltpu.SemaphoreType.DMA((4, n)),
            pltpu.SemaphoreType.DMA((2, n)),
            pltpu.SemaphoreType.DMA((2, n)),
            pltpu.SemaphoreType.DMA((4, n)),
            pltpu.SemaphoreType.DMA((2, n)),
            pltpu.SemaphoreType.DMA((2, nb)),
            pltpu.SemaphoreType.DMA((2, nb)),
            pltpu.SemaphoreType.DMA((2, n)),
            pltpu.SemaphoreType.DMA((2, nb)),
        ],
        compiler_params=pltpu.CompilerParams(
            collective_id=0, has_side_effects=True, vmem_limit_bytes=60 * 1024 * 1024
        ),
    )(
        q_rows,
        k_rows,
        turned,
        pre,
        wt,
        output_bias[:, None],
        key_pos,
        query_pos[:, None],
        live[:, None],
        live[None, :],
        lengths,
    )
    weight_grad = jnp.moveaxis(gw[:, :heads], 0, 1).reshape(heads, hidden).T
    return (grad, gb[0], weight_grad, gw[0, heads:, 0])


def solution(mesh):
    return jax.shard_map(
        on_device,
        mesh=mesh,
        in_specs=(
            P("batch", "seq", None),
            P("batch", "seq", None),
            P("batch", "seq", None),
            P("batch"),
            P("batch", None),
            P(),
            P(),
            P(),
            P(),
        ),
        out_specs=(P(("seq", "batch"), None), P(), P(), P()),
        check_vma=False,
    )
```

```python
import functools
import math

import jax
import jax.numpy as jnp
from jax import lax
from jax.experimental import pallas as pl
from jax.experimental.pallas import tpu as pltpu
from jax.sharding import PartitionSpec as P

F32 = jnp.float32
BF16 = jnp.bfloat16
MESH = pl.DeviceIdType.MESH


def copy_to(src, dst, send, recv, target):
    return pltpu.make_async_remote_copy(
        src_ref=src,
        dst_ref=dst,
        send_sem=send,
        recv_sem=recv,
        device_id=target,
        device_id_type=MESH,
    )


def kernel(
    n,
    nb,
    norm,
    scale,
    q_ref,
    k_ref,
    v_ref,
    w_ref,
    b_ref,
    wt_ref,
    bias_ref,
    order_ref,
    limit_ref,
    grad_ref,
    gb_ref,
    gw_ref,
    ob_ref,
    kg,
    ft,
    act,
    msum,
    mp,
    mr,
    delta,
    dg,
    otc,
    otr,
    obs,
    obr,
    ofin,
    dbs,
    dbr,
    cs,
    cr,
    ksem,
    fsem,
    msem,
    dsem,
    osem,
    bsem,
    gsem,
    hsem,
    csem,
    turned,
    weights_in,
    pre_ref,
    mask,
    wsem,
):
    me = lax.axis_index("seq")
    mb = lax.axis_index("batch")
    rows, kd = k_ref.shape
    heads = msum.shape[0]
    head = kd // heads
    per_group = q_ref.shape[1] // kd
    hidden = pre_ref.shape[1]
    load = pltpu.make_async_copy(w_ref, weights_in, wsem)
    load.start()
    inner = 2
    outer = n // inner
    mo = me // inner
    mi = me % inner
    pair = mo * inner + (inner - 1 - mi)

    def seq_peer(d):
        return lax.rem(me + d, n)

    def batch_peer(d):
        return lax.rem(mb + d, nb)

    def outer_peer(d):
        return lax.rem(mo + d, outer) * inner + mi

    def outer_source(d):
        return lax.rem(mo - d + outer, outer) * inner + mi

    barrier = pltpu.get_barrier_semaphore()
    for d in range(1, n):
        pl.semaphore_signal(barrier, inc=1, device_id={"seq": seq_peer(d)}, device_id_type=MESH)
    for d in range(1, nb):
        pl.semaphore_signal(
            barrier, inc=1, device_id={"batch": batch_peer(d)}, device_id_type=MESH
        )
    pl.semaphore_wait(barrier, n + nb - 2)

    def block(ref, owner):
        return ref.at[pl.ds(pl.multiple_of(owner * rows, rows), rows)]

    def gather_start(src, dst, sem):
        copies = []
        for d in range(1, outer):
            copy = copy_to(
                src, block(dst, me), sem.at[0, d], sem.at[1, d], {"seq": outer_peer(d)}
            )
            copy.start()
            copies.append(copy)
        copy = copy_to(src, block(dst, me), sem.at[2, 0], sem.at[3, 0], {"seq": pair})
        copy.start()
        return copies, [copy]

    def gather_finish(dst, sem, started):
        direct, passed = started
        for d in range(1, outer):
            direct[d - 1].wait_recv()
            held = block(dst, outer_source(d))
            copy = copy_to(held, held, sem.at[2, d], sem.at[3, d], {"seq": pair})
            copy.start()
            passed.append(copy)
        for copy in passed:
            copy.wait_recv()
        return direct + passed

    key_copies = gather_start(k_ref, kg, ksem)
    feat_copies = []
    cols = ft.shape[0]

    def send_features(first, last):
        for d in range(first, last):
            copy = copy_to(
                turned.at[pl.ds(pl.multiple_of(seq_peer(d) * cols, 16), cols)],
                ft.at[:, pl.ds(pl.multiple_of(me * rows, rows), rows)],
                fsem.at[0, d],
                fsem.at[1, d],
                {"seq": seq_peer(d)},
            )
            copy.start()
            feat_copies.append(copy)

    kg[pl.ds(pl.multiple_of(me * rows, rows), rows), :] = k_ref[...]
    base = 0
    for ref in (q_ref, k_ref, v_ref):

        def turn(c, carry, ref=ref, base=base):
            tile = ref[:, pl.ds(pl.multiple_of(c * head, head), head)]
            turned[pl.ds(pl.multiple_of(base + c * head, head), head), :] = tile.T
            return carry

        lax.fori_loop(0, ref.shape[1] // head, turn, 0)
        base += ref.shape[1]
    load.wait()
    tile_width = hidden // 4

    def project(c, carry):
        span = pl.ds(pl.multiple_of(c * tile_width, tile_width), tile_width)
        value = b_ref[:, span]
        base = 0
        for ref in (q_ref, k_ref, v_ref):
            depth = ref.shape[1]
            value = value + jnp.dot(
                ref[...], weights_in[base : base + depth, span], preferred_element_type=F32
            )
            base += depth
        pre_ref[:, span] = value
        act[:, span] = (value * jax.nn.sigmoid(value)).astype(BF16)
        return carry

    lax.fori_loop(0, 4, project, 0)
    ft[:, pl.ds(pl.multiple_of(me * rows, rows), rows)] = turned[
        pl.ds(pl.multiple_of(me * cols, 16), cols), :
    ]
    sent = gather_finish(kg, ksem, key_copies)
    early = n // 2
    send_features(1, early)

    limit = limit_ref[0]
    lane = lax.broadcasted_iota(jnp.int32, (1, rows), 1)
    key_pos = jnp.concatenate([lane + order_ref[0, p] * rows for p in range(n)], axis=1)
    query_start = order_ref[0, me] * rows
    query_pos = lax.broadcasted_iota(jnp.int32, (rows, 1), 0) + query_start
    live_col = (query_pos < limit).astype(F32)
    live_row = (lane + query_start < limit).astype(F32)
    allowed = (key_pos <= query_pos) & (key_pos < limit)
    mask[...] = jnp.where(allowed, 0.0, -1e30)

    def group(g, carry):
        keys = kg[:, pl.ds(pl.multiple_of(g * head, head), head)]
        hide = mask[...]
        column = jnp.zeros((1, n * rows), F32)
        for j in range(per_group):
            start = pl.multiple_of((g * per_group + j) * head, head)
            score = lax.dot_general(
                q_ref[:, pl.ds(start, head)],
                keys,
                (((1,), (1,)), ((), ())),
                preferred_element_type=F32,
            )
            masked = jnp.where(hide < 0.0, hide, score * scale)
            top = jnp.max(masked, axis=1, keepdims=True)
            weights = jnp.exp(masked - top)
            denom = jnp.sum(weights, axis=1, keepdims=True)
            column += jnp.sum(weights * (live_col / denom), axis=0, keepdims=True)
        msum[g] = column
        return carry

    lax.fori_loop(0, heads, group, 0)
    for p in range(n):
        mp[p] = msum[:, 0, p * rows : (p + 1) * rows]
    mass_copies = []
    for d in range(1, n):
        copy = copy_to(
            mp.at[seq_peer(d)], mr.at[d], msem.at[0, d], msem.at[1, d], {"seq": seq_peer(d)}
        )
        copy.start()
        mass_copies.append(copy)
    wt = wt_ref[...]
    pred = (
        lax.dot_general(wt, act[...], (((1,), (1,)), ((), ())), preferred_element_type=F32)[:heads]
        + bias_ref[...]
    )
    mass = mp[me]
    for d in range(1, n):
        mass_copies[d - 1].wait_recv()
        mass = mass + mr[d]
    sent += mass_copies
    resid = ((pred - jnp.log1p(mass)) * live_row * norm).astype(BF16)
    resid32 = resid.astype(F32)
    resid_all = jnp.concatenate([resid32, jnp.zeros_like(resid32)], axis=0)
    resid_t = resid_all.T.astype(BF16)
    back = jnp.dot(resid_t, wt, preferred_element_type=F32)
    pre = pre_ref[...]
    sig = jax.nn.sigmoid(pre)
    delta[...] = (back * sig * (1.0 + pre * (1.0 - sig))).astype(BF16)
    delta_copies = gather_start(delta, dg, dsem)
    send_features(early, n)
    dg[pl.ds(pl.multiple_of(me * rows, rows), rows), :] = delta[...]

    out_term = jnp.dot(resid_all.astype(BF16), act[...], preferred_element_type=F32)
    width = hidden // n
    bias_sum = jnp.broadcast_to(jnp.sum(resid32, axis=1, keepdims=True), (heads, width))
    for p in range(n):
        otc[p, :heads] = out_term[:heads, p * width : (p + 1) * width]
        otc[p, heads:] = bias_sum
    first = []
    for d in range(1, n):
        copy = copy_to(
            otc.at[seq_peer(d)], otr.at[d], osem.at[0, d], osem.at[1, d], {"seq": seq_peer(d)}
        )
        copy.start()
        first.append(copy)
    small = otc[me]
    for d in range(1, n):
        first[d - 1].wait_recv()
        small = small + otr[d]
    obs[...] = small
    second = []
    for d in range(1, nb):
        copy = copy_to(
            obs, obr.at[d], bsem.at[0, d], bsem.at[1, d], {"batch": batch_peer(d)}
        )
        copy.start()
        second.append(copy)

    sent += gather_finish(dg, dsem, delta_copies)
    for copy in feat_copies:
        copy.wait_recv()
    part = cs.shape[1]
    chunks = []
    for d in range(1, nb):
        start = pl.multiple_of(batch_peer(d) * part, 16)
        cs[d] = jnp.dot(ft[pl.ds(start, part), :], dg[...], preferred_element_type=F32)
        copy = copy_to(
            cs.at[d], cr.at[d], csem.at[0, d], csem.at[1, d], {"batch": batch_peer(d)}
        )
        copy.start()
        chunks.append(copy)
    dbs[...] = jnp.dot(jnp.ones((8, n * rows), BF16), dg[...], preferred_element_type=F32)
    sums = []
    for d in range(1, nb):
        copy = copy_to(
            dbs, dbr.at[d], gsem.at[0, d], gsem.at[1, d], {"batch": batch_peer(d)}
        )
        copy.start()
        sums.append(copy)

    small = obs[...]
    for d in range(1, nb):
        second[d - 1].wait_recv()
        small = small + obr[d]
    ofin[me] = small
    third = []
    for d in range(1, n):
        copy = copy_to(
            ofin.at[me], ofin.at[me], hsem.at[0, d], hsem.at[1, d], {"seq": seq_peer(d)}
        )
        copy.start()
        third.append(copy)
    start = pl.multiple_of(mb * part, 16)
    total = jnp.dot(ft[pl.ds(start, part), :], dg[...], preferred_element_type=F32)
    for d in range(1, nb):
        chunks[d - 1].wait_recv()
        total = total + cr[d]
    grad_ref[...] = total
    grad_b = dbs[...]
    for d in range(1, nb):
        sums[d - 1].wait_recv()
        grad_b = grad_b + dbr[d]
    gb_ref[...] = grad_b[:1]
    for copy in third:
        copy.wait_recv()
    gw_ref[...] = jnp.concatenate([ofin[p, :heads] for p in range(n)], axis=1).T
    ob_ref[...] = ofin[0, heads:, :1]
    for copy in sent + feat_copies + first + second + chunks + sums + third:
        copy.wait_send()


def on_device(queries, keys, values, lengths, block_pos, w_in, b_in, output_weight, output_bias):
    n = lax.axis_size("seq")
    nb = lax.axis_size("batch")
    q_rows = queries[0]
    k_rows = keys[0]
    v_rows = values[0]
    rows, kd = k_rows.shape
    heads = output_weight.shape[1]
    hidden = w_in.shape[1]
    feat = w_in.shape[0]
    cols = feat // n
    part = cols // nb
    scale = 1.0 / math.sqrt(kd // heads)
    norm = 1.0 / math.sqrt(nb * n * rows)
    wt = jnp.pad(output_weight.T, ((0, heads), (0, 0)))
    vmem = pl.BlockSpec(memory_space=pltpu.VMEM)
    total = n * rows
    width = hidden // n
    grad, gb, gw, ob = pl.pallas_call(
        functools.partial(kernel, n, nb, norm, scale),
        out_shape=(
            jax.ShapeDtypeStruct((part, hidden), F32),
            jax.ShapeDtypeStruct((1, hidden), F32),
            jax.ShapeDtypeStruct((hidden, heads), F32),
            jax.ShapeDtypeStruct((heads, 1), F32),
        ),
        in_specs=[vmem] * 3
        + [pl.BlockSpec(memory_space=pl.ANY)]
        + [vmem] * 3
        + [pl.BlockSpec(memory_space=pltpu.SMEM)] * 2,
        out_specs=(vmem, vmem, vmem, vmem),
        scratch_shapes=[
            pltpu.VMEM((total, kd), BF16),
            pltpu.VMEM((cols, total), BF16),
            pltpu.VMEM((rows, hidden), BF16),
            pltpu.VMEM((heads, 1, total), F32),
            pltpu.VMEM((n, heads, rows), F32),
            pltpu.VMEM((n, heads, rows), F32),
            pltpu.VMEM((rows, hidden), BF16),
            pltpu.VMEM((total, hidden), BF16),
            pltpu.VMEM((n, 2 * heads, width), F32),
            pltpu.VMEM((n, 2 * heads, width), F32),
            pltpu.VMEM((2 * heads, width), F32),
            pltpu.VMEM((nb, 2 * heads, width), F32),
            pltpu.VMEM((n, 2 * heads, width), F32),
            pltpu.VMEM((8, hidden), F32),
            pltpu.VMEM((nb, 8, hidden), F32),
            pltpu.VMEM((nb, part, hidden), F32),
            pltpu.VMEM((nb, part, hidden), F32),
            pltpu.SemaphoreType.DMA((4, n)),
            pltpu.SemaphoreType.DMA((2, n)),
            pltpu.SemaphoreType.DMA((2, n)),
            pltpu.SemaphoreType.DMA((4, n)),
            pltpu.SemaphoreType.DMA((2, n)),
            pltpu.SemaphoreType.DMA((2, nb)),
            pltpu.SemaphoreType.DMA((2, nb)),
            pltpu.SemaphoreType.DMA((2, n)),
            pltpu.SemaphoreType.DMA((2, nb)),
            pltpu.VMEM((feat, rows), BF16),
            pltpu.VMEM((feat, hidden), BF16),
            pltpu.VMEM((rows, hidden), F32),
            pltpu.VMEM((rows, total), F32),
            pltpu.SemaphoreType.DMA,
        ],
        compiler_params=pltpu.CompilerParams(
            collective_id=0, has_side_effects=True, vmem_limit_bytes=60 * 1024 * 1024
        ),
    )(
        q_rows,
        k_rows,
        v_rows,
        w_in,
        b_in[None, :],
        wt,
        output_bias[:, None],
        block_pos,
        lengths,
    )
    return (grad, gb[0], gw, ob[:, 0])


def solution(mesh):
    return jax.shard_map(
        on_device,
        mesh=mesh,
        in_specs=(
            P("batch", "seq", None),
            P("batch", "seq", None),
            P("batch", "seq", None),
            P("batch"),
            P("batch", None),
            P(),
            P(),
            P(),
            P(),
        ),
        out_specs=(P(("seq", "batch"), None), P(), P(), P()),
        check_vma=False,
    )
```

```python
import functools
import math

import jax
import jax.numpy as jnp
from jax import lax
from jax.experimental import pallas as pl
from jax.experimental.pallas import tpu as pltpu
from jax.sharding import PartitionSpec as P

F32 = jnp.float32
BF16 = jnp.bfloat16
PIECES = 2
MESH = pl.DeviceIdType.MESH


def copy_to(src, dst, send, recv, target):
    return pltpu.make_async_remote_copy(
        src_ref=src,
        dst_ref=dst,
        send_sem=send,
        recv_sem=recv,
        device_id=target,
        device_id_type=MESH,
    )


def kernel(
    n,
    nb,
    norm,
    scale,
    q_ref,
    k_ref,
    v_ref,
    w_ref,
    b_ref,
    wt_ref,
    bias_ref,
    order_ref,
    limit_ref,
    grad_ref,
    gb_ref,
    gw_ref,
    ob_ref,
    kg,
    ft,
    act,
    msum,
    mp,
    mr,
    delta,
    dg,
    otc,
    otr,
    obs,
    obr,
    ofin,
    dbs,
    dbr,
    cs,
    cr,
    ksem,
    fsem,
    msem,
    dsem,
    osem,
    bsem,
    gsem,
    hsem,
    csem,
    turned,
    weights_in,
    pre_ref,
    mask,
    ns,
    nr,
    nsem,
    wsem,
):
    me = lax.axis_index("seq")
    mb = lax.axis_index("batch")
    rows, kd = k_ref.shape
    heads = msum.shape[0]
    head = kd // heads
    per_group = q_ref.shape[1] // kd
    hidden = pre_ref.shape[1]
    load = pltpu.make_async_copy(w_ref, weights_in, wsem)
    load.start()
    inner = 2
    outer = n // inner
    mo = me // inner
    mi = me % inner
    pair = mo * inner + (inner - 1 - mi)

    def seq_peer(d):
        return lax.rem(me + d, n)

    def batch_peer(d):
        return lax.rem(mb + d, nb)

    def outer_peer(d):
        return lax.rem(mo + d, outer) * inner + mi

    def outer_source(d):
        return lax.rem(mo - d + outer, outer) * inner + mi

    barrier = pltpu.get_barrier_semaphore()
    for d in range(1, n):
        pl.semaphore_signal(barrier, inc=1, device_id={"seq": seq_peer(d)}, device_id_type=MESH)
    for d in range(1, nb):
        pl.semaphore_signal(
            barrier, inc=1, device_id={"batch": batch_peer(d)}, device_id_type=MESH
        )
    pl.semaphore_wait(barrier, n + nb - 2)

    def block(ref, owner):
        return ref.at[pl.ds(pl.multiple_of(owner * rows, rows), rows)]

    def gather_start(src, dst, sem):
        copies = []
        for d in range(1, outer):
            copy = copy_to(
                src, block(dst, me), sem.at[0, d], sem.at[1, d], {"seq": outer_peer(d)}
            )
            copy.start()
            copies.append(copy)
        copy = copy_to(src, block(dst, me), sem.at[2, 0], sem.at[3, 0], {"seq": pair})
        copy.start()
        return copies, [copy]

    def gather_finish(dst, sem, started):
        direct, passed = started
        for d in range(1, outer):
            direct[d - 1].wait_recv()
            held = block(dst, outer_source(d))
            copy = copy_to(held, held, sem.at[2, d], sem.at[3, d], {"seq": pair})
            copy.start()
            passed.append(copy)
        for copy in passed:
            copy.wait_recv()
        return direct + passed

    key_copies = gather_start(k_ref, kg, ksem)
    feat_copies = []
    cols = ft.shape[0]

    def send_features(first, last):
        for d in range(first, last):
            copy = copy_to(
                turned.at[pl.ds(pl.multiple_of(seq_peer(d) * cols, 16), cols)],
                ft.at[:, pl.ds(pl.multiple_of(me * rows, rows), rows)],
                fsem.at[0, d],
                fsem.at[1, d],
                {"seq": seq_peer(d)},
            )
            copy.start()
            feat_copies.append(copy)

    kg[pl.ds(pl.multiple_of(me * rows, rows), rows), :] = k_ref[...]
    base = 0
    for ref in (q_ref, k_ref, v_ref):

        def turn(c, carry, ref=ref, base=base):
            tile = ref[:, pl.ds(pl.multiple_of(c * head, head), head)]
            turned[pl.ds(pl.multiple_of(base + c * head, head), head), :] = tile.T
            return carry

        lax.fori_loop(0, ref.shape[1] // head, turn, 0)
        base += ref.shape[1]
    load.wait()
    tile_width = hidden // 4

    def project(c, carry):
        span = pl.ds(pl.multiple_of(c * tile_width, tile_width), tile_width)
        value = b_ref[:, span]
        base = 0
        for ref in (q_ref, k_ref, v_ref):
            depth = ref.shape[1]
            value = value + jnp.dot(
                ref[...], weights_in[base : base + depth, span], preferred_element_type=F32
            )
            base += depth
        pre_ref[:, span] = value
        act[:, span] = (value * jax.nn.sigmoid(value)).astype(BF16)
        return carry

    lax.fori_loop(0, 4, project, 0)
    ft[:, pl.ds(pl.multiple_of(me * rows, rows), rows)] = turned[
        pl.ds(pl.multiple_of(me * cols, 16), cols), :
    ]
    sent = gather_finish(kg, ksem, key_copies)
    early = n
    send_features(1, early)

    limit = limit_ref[0]
    lane = lax.broadcasted_iota(jnp.int32, (1, rows), 1)
    key_pos = jnp.concatenate([lane + order_ref[0, p] * rows for p in range(n)], axis=1)
    query_start = order_ref[0, me] * rows
    query_pos = lax.broadcasted_iota(jnp.int32, (rows, 1), 0) + query_start
    live_col = (query_pos < limit).astype(F32)
    live_row = (lane + query_start < limit).astype(F32)
    allowed = (key_pos <= query_pos) & (key_pos < limit)
    mask[...] = jnp.where(allowed, 0.0, -1e30)

    def group(g, carry):
        keys = kg[:, pl.ds(pl.multiple_of(g * head, head), head)]
        hide = mask[...]
        column = jnp.zeros((1, n * rows), F32)
        for j in range(per_group):
            start = pl.multiple_of((g * per_group + j) * head, head)
            score = lax.dot_general(
                q_ref[:, pl.ds(start, head)],
                keys,
                (((1,), (1,)), ((), ())),
                preferred_element_type=F32,
            )
            masked = jnp.where(hide < 0.0, hide, score * scale)
            top = jnp.max(masked, axis=1, keepdims=True)
            weights = jnp.exp(masked - top)
            denom = jnp.sum(weights, axis=1, keepdims=True)
            column += jnp.sum(weights * (live_col / denom), axis=0, keepdims=True)
        msum[g] = column
        return carry

    lax.fori_loop(0, heads, group, 0)
    for p in range(n):
        mp[p] = msum[:, 0, p * rows : (p + 1) * rows]
    mass_copies = []
    for d in range(1, n):
        copy = copy_to(
            mp.at[seq_peer(d)], mr.at[d], msem.at[0, d], msem.at[1, d], {"seq": seq_peer(d)}
        )
        copy.start()
        mass_copies.append(copy)
    wt = wt_ref[...]
    pred = (
        lax.dot_general(wt, act[...], (((1,), (1,)), ((), ())), preferred_element_type=F32)[:heads]
        + bias_ref[...]
    )
    mass = mp[me]
    for d in range(1, n):
        mass_copies[d - 1].wait_recv()
        mass = mass + mr[d]
    sent += mass_copies
    resid = ((pred - jnp.log1p(mass)) * live_row * norm).astype(BF16)
    resid32 = resid.astype(F32)
    resid_all = jnp.concatenate([resid32, jnp.zeros_like(resid32)], axis=0)
    resid_t = resid_all.T.astype(BF16)
    back = jnp.dot(resid_t, wt, preferred_element_type=F32)
    pre = pre_ref[...]
    sig = jax.nn.sigmoid(pre)
    slope = (back * sig * (1.0 + pre * (1.0 - sig))).astype(BF16)
    piece = hidden // PIECES
    delta_copies = []
    for h in range(PIECES):
        delta[h] = slope[:, h * piece : (h + 1) * piece]
        delta_copies.append(gather_start(delta.at[h], dg.at[h], dsem.at[h]))
        if h == 0:
            send_features(early, n)
        dg[h, pl.ds(pl.multiple_of(me * rows, rows), rows), :] = delta[h]

    out_term = jnp.dot(resid_all.astype(BF16), act[...], preferred_element_type=F32)
    width = hidden // n
    bias_sum = jnp.broadcast_to(jnp.sum(resid32, axis=1, keepdims=True), (heads, width))
    for p in range(n):
        otc[p, :heads] = out_term[:heads, p * width : (p + 1) * width]
        otc[p, heads:] = bias_sum
    first = []
    for d in range(1, n):
        copy = copy_to(
            otc.at[seq_peer(d)], otr.at[d], osem.at[0, d], osem.at[1, d], {"seq": seq_peer(d)}
        )
        copy.start()
        first.append(copy)
    small = otc[me]
    for d in range(1, n):
        first[d - 1].wait_recv()
        small = small + otr[d]
    obs[...] = small
    second = []
    for d in range(1, nb):
        copy = copy_to(
            obs, obr.at[d], bsem.at[0, d], bsem.at[1, d], {"batch": batch_peer(d)}
        )
        copy.start()
        second.append(copy)

    part = cr.shape[2]
    bo = mb // inner
    bi = mb % inner
    bouter = nb // inner
    twin = bo * inner + (inner - 1 - bi)

    def term(h, owner):
        start = pl.multiple_of(owner * part, 16)
        return jnp.dot(ft[pl.ds(start, part), :], dg[h], preferred_element_type=F32)

    chunks = []
    near = []
    for h in range(PIECES):
        sent += gather_finish(dg.at[h], dsem.at[h], delta_copies[h])
        if h == 0:
            for copy in feat_copies:
                copy.wait_recv()
        swaps = []
        for e in range(bouter):
            ahead = lax.rem(bo + 1 + e, bouter)
            ns[h, e] = term(h, ahead * inner + (inner - 1 - bi))
            copy = copy_to(
                ns.at[h, e], nr.at[h, e], nsem.at[0, h, e], nsem.at[1, h, e], {"batch": twin}
            )
            copy.start()
            swaps.append(copy)
        near += swaps
        for e in range(bouter):
            ahead = lax.rem(bo + 1 + e, bouter)
            value = term(h, ahead * inner + bi)
            swaps[e].wait_recv()
            value = value + nr[h, e]
            if e == bouter - 1:
                grad_ref[:, h * piece : (h + 1) * piece] = value
            else:
                cs[h, e] = value
                copy = copy_to(
                    cs.at[h, e],
                    cr.at[h, e],
                    csem.at[0, h, e],
                    csem.at[1, h, e],
                    {"batch": ahead * inner + bi},
                )
                copy.start()
                chunks.append((h, e, copy))
        dbs[:, h * piece : (h + 1) * piece] = jnp.dot(
            jnp.ones((8, n * rows), BF16), dg[h], preferred_element_type=F32
        )
    sums = []
    for d in range(1, nb):
        copy = copy_to(
            dbs, dbr.at[d], gsem.at[0, d], gsem.at[1, d], {"batch": batch_peer(d)}
        )
        copy.start()
        sums.append(copy)

    small = obs[...]
    for d in range(1, nb):
        second[d - 1].wait_recv()
        small = small + obr[d]
    ofin[me] = small
    third = []
    for d in range(1, n):
        copy = copy_to(
            ofin.at[me], ofin.at[me], hsem.at[0, d], hsem.at[1, d], {"seq": seq_peer(d)}
        )
        copy.start()
        third.append(copy)
    for h, e, copy in chunks:
        copy.wait_recv()
        grad_ref[:, h * piece : (h + 1) * piece] += cr[h, e]
    grad_b = dbs[...]
    for d in range(1, nb):
        sums[d - 1].wait_recv()
        grad_b = grad_b + dbr[d]
    gb_ref[...] = grad_b[:1]
    for copy in third:
        copy.wait_recv()
    gw_ref[...] = jnp.concatenate([ofin[p, :heads] for p in range(n)], axis=1).T
    ob_ref[...] = ofin[0, heads:, :1]
    for copy in sent + feat_copies + first + second + near + sums + third + [c[2] for c in chunks]:
        copy.wait_send()


def on_device(queries, keys, values, lengths, block_pos, w_in, b_in, output_weight, output_bias):
    n = lax.axis_size("seq")
    nb = lax.axis_size("batch")
    q_rows = queries[0]
    k_rows = keys[0]
    v_rows = values[0]
    rows, kd = k_rows.shape
    heads = output_weight.shape[1]
    hidden = w_in.shape[1]
    feat = w_in.shape[0]
    cols = feat // n
    part = cols // nb
    scale = 1.0 / math.sqrt(kd // heads)
    norm = 1.0 / math.sqrt(nb * n * rows)
    wt = jnp.pad(output_weight.T, ((0, heads), (0, 0)))
    vmem = pl.BlockSpec(memory_space=pltpu.VMEM)
    total = n * rows
    width = hidden // n
    grad, gb, gw, ob = pl.pallas_call(
        functools.partial(kernel, n, nb, norm, scale),
        out_shape=(
            jax.ShapeDtypeStruct((part, hidden), F32),
            jax.ShapeDtypeStruct((1, hidden), F32),
            jax.ShapeDtypeStruct((hidden, heads), F32),
            jax.ShapeDtypeStruct((heads, 1), F32),
        ),
        in_specs=[vmem] * 3
        + [pl.BlockSpec(memory_space=pl.ANY)]
        + [vmem] * 3
        + [pl.BlockSpec(memory_space=pltpu.SMEM)] * 2,
        out_specs=(vmem, vmem, vmem, vmem),
        scratch_shapes=[
            pltpu.VMEM((total, kd), BF16),
            pltpu.VMEM((cols, total), BF16),
            pltpu.VMEM((rows, hidden), BF16),
            pltpu.VMEM((heads, 1, total), F32),
            pltpu.VMEM((n, heads, rows), F32),
            pltpu.VMEM((n, heads, rows), F32),
            pltpu.VMEM((PIECES, rows, hidden // PIECES), BF16),
            pltpu.VMEM((PIECES, total, hidden // PIECES), BF16),
            pltpu.VMEM((n, 2 * heads, width), F32),
            pltpu.VMEM((n, 2 * heads, width), F32),
            pltpu.VMEM((2 * heads, width), F32),
            pltpu.VMEM((nb, 2 * heads, width), F32),
            pltpu.VMEM((n, 2 * heads, width), F32),
            pltpu.VMEM((8, hidden), F32),
            pltpu.VMEM((nb, 8, hidden), F32),
            pltpu.VMEM((PIECES, nb // 2, part, hidden // PIECES), F32),
            pltpu.VMEM((PIECES, nb // 2, part, hidden // PIECES), F32),
            pltpu.SemaphoreType.DMA((4, n)),
            pltpu.SemaphoreType.DMA((2, n)),
            pltpu.SemaphoreType.DMA((2, n)),
            pltpu.SemaphoreType.DMA((PIECES, 4, n)),
            pltpu.SemaphoreType.DMA((2, n)),
            pltpu.SemaphoreType.DMA((2, nb)),
            pltpu.SemaphoreType.DMA((2, nb)),
            pltpu.SemaphoreType.DMA((2, n)),
            pltpu.SemaphoreType.DMA((2, PIECES, nb)),
            pltpu.VMEM((feat, rows), BF16),
            pltpu.VMEM((feat, hidden), BF16),
            pltpu.VMEM((rows, hidden), F32),
            pltpu.VMEM((rows, total), F32),
            pltpu.VMEM((PIECES, nb // 2, part, hidden // PIECES), F32),
            pltpu.VMEM((PIECES, nb // 2, part, hidden // PIECES), F32),
            pltpu.SemaphoreType.DMA((2, PIECES, nb)),
            pltpu.SemaphoreType.DMA,
        ],
        compiler_params=pltpu.CompilerParams(
            collective_id=0, has_side_effects=True, vmem_limit_bytes=60 * 1024 * 1024
        ),
    )(
        q_rows,
        k_rows,
        v_rows,
        w_in,
        b_in[None, :],
        wt,
        output_bias[:, None],
        block_pos,
        lengths,
    )
    return (grad, gb[0], gw, ob[:, 0])


def solution(mesh):
    return jax.shard_map(
        on_device,
        mesh=mesh,
        in_specs=(
            P("batch", "seq", None),
            P("batch", "seq", None),
            P("batch", "seq", None),
            P("batch"),
            P("batch", None),
            P(),
            P(),
            P(),
            P(),
        ),
        out_specs=(P(("seq", "batch"), None), P(), P(), P()),
        check_vma=False,
    )
```

```python
import functools
import math

import jax
import jax.numpy as jnp
from jax import lax
from jax.experimental import pallas as pl
from jax.experimental.pallas import tpu as pltpu
from jax.sharding import PartitionSpec as P

F32 = jnp.float32
BF16 = jnp.bfloat16
PIECES = 2
MESH = pl.DeviceIdType.MESH


def copy_to(src, dst, send, recv, target):
    return pltpu.make_async_remote_copy(
        src_ref=src,
        dst_ref=dst,
        send_sem=send,
        recv_sem=recv,
        device_id=target,
        device_id_type=MESH,
    )


def kernel(
    n,
    nb,
    norm,
    scale,
    q_ref,
    k_ref,
    v_ref,
    w_ref,
    b_ref,
    wt_ref,
    bias_ref,
    order_ref,
    limit_ref,
    grad_ref,
    gb_ref,
    gw_ref,
    ob_ref,
    kg,
    ft,
    act,
    msum,
    mp,
    mr,
    delta,
    dg,
    otc,
    otr,
    obs,
    obr,
    ofin,
    dbs,
    dbr,
    cs,
    cr,
    ksem,
    fsem,
    msem,
    dsem,
    osem,
    bsem,
    gsem,
    hsem,
    csem,
    turned,
    weights_in,
    pre_ref,
    mask,
    ns,
    nr,
    nsem,
    wsem,
):
    me = lax.axis_index("seq")
    mb = lax.axis_index("batch")
    rows, kd = k_ref.shape
    heads = msum.shape[0]
    head = kd // heads
    per_group = q_ref.shape[1] // kd
    hidden = pre_ref.shape[1]
    load = pltpu.make_async_copy(w_ref, weights_in, wsem)
    load.start()
    inner = 2
    outer = n // inner
    mo = me // inner
    mi = me % inner
    pair = mo * inner + (inner - 1 - mi)

    def seq_peer(d):
        return lax.rem(me + d, n)

    def batch_peer(d):
        return lax.rem(mb + d, nb)

    def outer_peer(d):
        return lax.rem(mo + d, outer) * inner + mi

    def outer_source(d):
        return lax.rem(mo - d + outer, outer) * inner + mi

    barrier = pltpu.get_barrier_semaphore()
    for d in range(1, n):
        pl.semaphore_signal(barrier, inc=1, device_id={"seq": seq_peer(d)}, device_id_type=MESH)
    for d in range(1, nb):
        pl.semaphore_signal(
            barrier, inc=1, device_id={"batch": batch_peer(d)}, device_id_type=MESH
        )
    pl.semaphore_wait(barrier, n + nb - 2)

    def block(ref, owner):
        return ref.at[pl.ds(pl.multiple_of(owner * rows, rows), rows)]

    def gather_start(src, dst, sem):
        copies = []
        for d in range(1, outer):
            copy = copy_to(
                src, block(dst, me), sem.at[0, d], sem.at[1, d], {"seq": outer_peer(d)}
            )
            copy.start()
            copies.append(copy)
        copy = copy_to(src, block(dst, me), sem.at[2, 0], sem.at[3, 0], {"seq": pair})
        copy.start()
        return copies, [copy]

    def gather_finish(dst, sem, started, follow=None):
        direct, passed = started
        for d in range(1, outer):
            direct[d - 1].wait_recv()
            held = block(dst, outer_source(d))
            copy = copy_to(held, held, sem.at[2, d], sem.at[3, d], {"seq": pair})
            copy.start()
            passed.append(copy)
        if follow is not None:
            follow()
        for copy in passed:
            copy.wait_recv()
        return direct + passed

    key_copies = gather_start(k_ref, kg, ksem)
    feat_copies = []
    cols = ft.shape[0]

    def send_features(first, last):
        for d in range(first, last):
            copy = copy_to(
                turned.at[pl.ds(pl.multiple_of(seq_peer(d) * cols, 16), cols)],
                ft.at[:, pl.ds(pl.multiple_of(me * rows, rows), rows)],
                fsem.at[0, d],
                fsem.at[1, d],
                {"seq": seq_peer(d)},
            )
            copy.start()
            feat_copies.append(copy)

    kg[pl.ds(pl.multiple_of(me * rows, rows), rows), :] = k_ref[...]
    base = 0
    for ref in (q_ref, k_ref, v_ref):

        def turn(c, carry, ref=ref, base=base):
            tile = ref[:, pl.ds(pl.multiple_of(c * head, head), head)]
            turned[pl.ds(pl.multiple_of(base + c * head, head), head), :] = tile.T
            return carry

        lax.fori_loop(0, ref.shape[1] // head, turn, 0)
        base += ref.shape[1]
    load.wait()
    tile_width = hidden // 4

    def project(c, carry):
        span = pl.ds(pl.multiple_of(c * tile_width, tile_width), tile_width)
        value = b_ref[:, span]
        base = 0
        for ref in (q_ref, k_ref, v_ref):
            depth = ref.shape[1]
            value = value + jnp.dot(
                ref[...], weights_in[base : base + depth, span], preferred_element_type=F32
            )
            base += depth
        pre_ref[:, span] = value
        act[:, span] = (value * jax.nn.sigmoid(value)).astype(BF16)
        return carry

    lax.fori_loop(0, 4, project, 0)
    ft[:, pl.ds(pl.multiple_of(me * rows, rows), rows)] = turned[
        pl.ds(pl.multiple_of(me * cols, 16), cols), :
    ]
    sent = gather_finish(kg, ksem, key_copies, lambda: send_features(1, n))

    limit = limit_ref[0]
    lane = lax.broadcasted_iota(jnp.int32, (1, rows), 1)
    key_pos = jnp.concatenate([lane + order_ref[0, p] * rows for p in range(n)], axis=1)
    query_start = order_ref[0, me] * rows
    query_pos = lax.broadcasted_iota(jnp.int32, (rows, 1), 0) + query_start
    live_col = (query_pos < limit).astype(F32)
    live_row = (lane + query_start < limit).astype(F32)
    allowed = (key_pos <= query_pos) & (key_pos < limit)
    mask[...] = jnp.where(allowed, 0.0, -1e30)

    def group(g, carry):
        keys = kg[:, pl.ds(pl.multiple_of(g * head, head), head)]
        hide = mask[...]
        column = jnp.zeros((1, n * rows), F32)
        for j in range(per_group):
            start = pl.multiple_of((g * per_group + j) * head, head)
            score = lax.dot_general(
                q_ref[:, pl.ds(start, head)],
                keys,
                (((1,), (1,)), ((), ())),
                preferred_element_type=F32,
            )
            masked = jnp.where(hide < 0.0, hide, score * scale)
            top = jnp.max(masked, axis=1, keepdims=True)
            weights = jnp.exp(masked - top)
            denom = jnp.sum(weights, axis=1, keepdims=True)
            column += jnp.sum(weights * (live_col / denom), axis=0, keepdims=True)
        msum[g] = column
        return carry

    lax.fori_loop(0, heads, group, 0)
    for p in range(n):
        mp[p] = msum[:, 0, p * rows : (p + 1) * rows]
    mass_copies = []
    for d in range(1, n):
        copy = copy_to(
            mp.at[seq_peer(d)], mr.at[d], msem.at[0, d], msem.at[1, d], {"seq": seq_peer(d)}
        )
        copy.start()
        mass_copies.append(copy)
    wt = wt_ref[...]
    pred = (
        lax.dot_general(wt, act[...], (((1,), (1,)), ((), ())), preferred_element_type=F32)[:heads]
        + bias_ref[...]
    )
    mass = mp[me]
    for d in range(1, n):
        mass_copies[d - 1].wait_recv()
        mass = mass + mr[d]
    sent += mass_copies
    resid = ((pred - jnp.log1p(mass)) * live_row * norm).astype(BF16)
    resid32 = resid.astype(F32)
    resid_all = jnp.concatenate([resid32, jnp.zeros_like(resid32)], axis=0)
    resid_t = resid_all.T.astype(BF16)
    back = jnp.dot(resid_t, wt, preferred_element_type=F32)
    pre = pre_ref[...]
    sig = jax.nn.sigmoid(pre)
    slope = (back * sig * (1.0 + pre * (1.0 - sig))).astype(BF16)
    piece = hidden // PIECES
    delta_copies = []
    for h in range(PIECES):
        delta[h] = slope[:, h * piece : (h + 1) * piece]
        delta_copies.append(gather_start(delta.at[h], dg.at[h], dsem.at[h]))
        dg[h, pl.ds(pl.multiple_of(me * rows, rows), rows), :] = delta[h]

    out_term = jnp.dot(resid_all.astype(BF16), act[...], preferred_element_type=F32)
    width = hidden // n
    bias_sum = jnp.broadcast_to(jnp.sum(resid32, axis=1, keepdims=True), (heads, width))
    for p in range(n):
        otc[p, :heads] = out_term[:heads, p * width : (p + 1) * width]
        otc[p, heads:] = bias_sum
    first = []
    for d in range(1, n):
        copy = copy_to(
            otc.at[seq_peer(d)], otr.at[d], osem.at[0, d], osem.at[1, d], {"seq": seq_peer(d)}
        )
        copy.start()
        first.append(copy)
    small = otc[me]
    for d in range(1, n):
        first[d - 1].wait_recv()
        small = small + otr[d]
    obs[...] = small
    second = []
    for d in range(1, nb):
        copy = copy_to(
            obs, obr.at[d], bsem.at[0, d], bsem.at[1, d], {"batch": batch_peer(d)}
        )
        copy.start()
        second.append(copy)

    part = cr.shape[2]
    bo = mb // inner
    bi = mb % inner
    bouter = nb // inner
    twin = bo * inner + (inner - 1 - bi)

    def term(h, owner):
        start = pl.multiple_of(owner * part, 16)
        return jnp.dot(ft[pl.ds(start, part), :], dg[h], preferred_element_type=F32)

    chunks = []
    near = []
    for h in range(PIECES):
        sent += gather_finish(dg.at[h], dsem.at[h], delta_copies[h])
        if h == 0:
            for copy in feat_copies:
                copy.wait_recv()
        swaps = []
        for e in range(bouter):
            ahead = lax.rem(bo + 1 + e, bouter)
            ns[h, e] = term(h, ahead * inner + (inner - 1 - bi))
            copy = copy_to(
                ns.at[h, e], nr.at[h, e], nsem.at[0, h, e], nsem.at[1, h, e], {"batch": twin}
            )
            copy.start()
            swaps.append(copy)
        near += swaps
        for e in range(bouter):
            ahead = lax.rem(bo + 1 + e, bouter)
            value = term(h, ahead * inner + bi)
            swaps[e].wait_recv()
            value = value + nr[h, e]
            if e == bouter - 1:
                grad_ref[:, h * piece : (h + 1) * piece] = value
            else:
                cs[h, e] = value
                copy = copy_to(
                    cs.at[h, e],
                    cr.at[h, e],
                    csem.at[0, h, e],
                    csem.at[1, h, e],
                    {"batch": ahead * inner + bi},
                )
                copy.start()
                chunks.append((h, e, copy))
        dbs[:, h * piece : (h + 1) * piece] = jnp.dot(
            jnp.ones((8, n * rows), BF16), dg[h], preferred_element_type=F32
        )
    sums = []
    for d in range(1, nb):
        copy = copy_to(
            dbs, dbr.at[d], gsem.at[0, d], gsem.at[1, d], {"batch": batch_peer(d)}
        )
        copy.start()
        sums.append(copy)

    small = obs[...]
    for d in range(1, nb):
        second[d - 1].wait_recv()
        small = small + obr[d]
    ofin[me] = small
    third = []
    for d in range(1, n):
        copy = copy_to(
            ofin.at[me], ofin.at[me], hsem.at[0, d], hsem.at[1, d], {"seq": seq_peer(d)}
        )
        copy.start()
        third.append(copy)
    for h, e, copy in chunks:
        copy.wait_recv()
        grad_ref[:, h * piece : (h + 1) * piece] += cr[h, e]
    grad_b = dbs[...]
    for d in range(1, nb):
        sums[d - 1].wait_recv()
        grad_b = grad_b + dbr[d]
    gb_ref[...] = grad_b[:1]
    for copy in third:
        copy.wait_recv()
    gw_ref[...] = jnp.concatenate([ofin[p, :heads] for p in range(n)], axis=1).T
    ob_ref[...] = ofin[0, heads:, :1]
    for copy in sent + feat_copies + first + second + near + sums + third + [c[2] for c in chunks]:
        copy.wait_send()


def on_device(queries, keys, values, lengths, block_pos, w_in, b_in, output_weight, output_bias):
    n = lax.axis_size("seq")
    nb = lax.axis_size("batch")
    q_rows = queries[0]
    k_rows = keys[0]
    v_rows = values[0]
    rows, kd = k_rows.shape
    heads = output_weight.shape[1]
    hidden = w_in.shape[1]
    feat = w_in.shape[0]
    cols = feat // n
    part = cols // nb
    scale = 1.0 / math.sqrt(kd // heads)
    norm = 1.0 / math.sqrt(nb * n * rows)
    wt = jnp.pad(output_weight.T, ((0, heads), (0, 0)))
    vmem = pl.BlockSpec(memory_space=pltpu.VMEM)
    total = n * rows
    width = hidden // n
    grad, gb, gw, ob = pl.pallas_call(
        functools.partial(kernel, n, nb, norm, scale),
        out_shape=(
            jax.ShapeDtypeStruct((part, hidden), F32),
            jax.ShapeDtypeStruct((1, hidden), F32),
            jax.ShapeDtypeStruct((hidden, heads), F32),
            jax.ShapeDtypeStruct((heads, 1), F32),
        ),
        in_specs=[vmem] * 3
        + [pl.BlockSpec(memory_space=pl.ANY)]
        + [vmem] * 3
        + [pl.BlockSpec(memory_space=pltpu.SMEM)] * 2,
        out_specs=(vmem, vmem, vmem, vmem),
        scratch_shapes=[
            pltpu.VMEM((total, kd), BF16),
            pltpu.VMEM((cols, total), BF16),
            pltpu.VMEM((rows, hidden), BF16),
            pltpu.VMEM((heads, 1, total), F32),
            pltpu.VMEM((n, heads, rows), F32),
            pltpu.VMEM((n, heads, rows), F32),
            pltpu.VMEM((PIECES, rows, hidden // PIECES), BF16),
            pltpu.VMEM((PIECES, total, hidden // PIECES), BF16),
            pltpu.VMEM((n, 2 * heads, width), F32),
            pltpu.VMEM((n, 2 * heads, width), F32),
            pltpu.VMEM((2 * heads, width), F32),
            pltpu.VMEM((nb, 2 * heads, width), F32),
            pltpu.VMEM((n, 2 * heads, width), F32),
            pltpu.VMEM((8, hidden), F32),
            pltpu.VMEM((nb, 8, hidden), F32),
            pltpu.VMEM((PIECES, nb // 2, part, hidden // PIECES), F32),
            pltpu.VMEM((PIECES, nb // 2, part, hidden // PIECES), F32),
            pltpu.SemaphoreType.DMA((4, n)),
            pltpu.SemaphoreType.DMA((2, n)),
            pltpu.SemaphoreType.DMA((2, n)),
            pltpu.SemaphoreType.DMA((PIECES, 4, n)),
            pltpu.SemaphoreType.DMA((2, n)),
            pltpu.SemaphoreType.DMA((2, nb)),
            pltpu.SemaphoreType.DMA((2, nb)),
            pltpu.SemaphoreType.DMA((2, n)),
            pltpu.SemaphoreType.DMA((2, PIECES, nb)),
            pltpu.VMEM((feat, rows), BF16),
            pltpu.VMEM((feat, hidden), BF16),
            pltpu.VMEM((rows, hidden), F32),
            pltpu.VMEM((rows, total), F32),
            pltpu.VMEM((PIECES, nb // 2, part, hidden // PIECES), F32),
            pltpu.VMEM((PIECES, nb // 2, part, hidden // PIECES), F32),
            pltpu.SemaphoreType.DMA((2, PIECES, nb)),
            pltpu.SemaphoreType.DMA,
        ],
        compiler_params=pltpu.CompilerParams(
            collective_id=0, has_side_effects=True, vmem_limit_bytes=60 * 1024 * 1024
        ),
    )(
        q_rows,
        k_rows,
        v_rows,
        w_in,
        b_in[None, :],
        wt,
        output_bias[:, None],
        block_pos,
        lengths,
    )
    return (grad, gb[0], gw, ob[:, 0])


def solution(mesh):
    return jax.shard_map(
        on_device,
        mesh=mesh,
        in_specs=(
            P("batch", "seq", None),
            P("batch", "seq", None),
            P("batch", "seq", None),
            P("batch"),
            P("batch", None),
            P(),
            P(),
            P(),
            P(),
        ),
        out_specs=(P(("seq", "batch"), None), P(), P(), P()),
        check_vma=False,
    )
```
